32 devices in a mesh: dp: 4 (over z), neg: 8 (over y, x, core).
Axes of the slice: x: 2, y: 2, z: 4, core: 2. Of those that a mesh axis runs over, the one named last changes fastest.
Arguments:
- query_emb: bfloat16 [128, 32, 128], P(('dp', 'neg')), may hold values from -6 to 6
- positive: int32 [128], P(('dp', 'neg')), may hold values from 0 to 31
- passage_emb: bfloat16 [32, 512, 128], P(('dp', 'neg')), may hold values from -6 to 6
- lengths: int32 [32], P(('dp', 'neg')), may hold values from 256 to 512
- residual: bfloat16 [16384, 1024], P(('dp', 'neg')), may hold values from -6 to 6
- context: bfloat16 [16384, 1024], P(('dp', 'neg')), may hold values from -6 to 6
- out_proj: bfloat16 [1024, 1024], replicated, may hold values from -0.1875 to 0.1875
- norm_gain: float32 [1024], replicated, may hold values from 0.5 to 1.5
- colbert_proj: bfloat16 [1024, 128], replicated, may hold values from -0.1875 to 0.1875
Outputs:
- loss: float32 [], replicated
- query_grad: float32 [128, 32, 128], P(('dp', 'neg'))
- residual_grad: bfloat16 [16384, 1024], P(('dp', 'neg'))
- context_grad: bfloat16 [16384, 1024], P(('dp', 'neg'))
- out_proj_grad: float32 [1024, 1024], replicated
- colbert_grad: float32 [1024, 128], replicated
- gain_grad: float32 [1024], replicated
The draws below stay inside these ranges and needn't reach their ends.
Inputs may be any that keep to these rules, and one draw needn't show every extreme that they name: A passage's first lengths[p] token slots are real, the rest padding.
All inputs are finite; a program needn't handle non-finite values.
Results may differ from the reference program's by a relative error of at most 0.0065.
Values may be sent and summed in bfloat16 or wider, within the bound.
A program may use at most 64 MiB of HBM per device.

```python
import jax
import jax.numpy as jnp
from jax import lax

D = 1024
DIM = 128
QLEN = 32
PLEN = 512
QUERIES = 128
PASSAGES = 32
ROWS = 16384


noise_level = 0.6


similar_gap = 9.5


def unit_rows(values):
    return values / jnp.sqrt(jnp.sum(values * values, axis=-1, keepdims=True))


def shared_parts(key):
    midpoint = DIM // 2
    first_half = (jnp.arange(DIM) < midpoint).astype(jnp.float32)
    second_half = 1.0 - first_half
    chosen = jax.random.randint(jax.random.fold_in(key, 101), (QUERIES,), 0, PASSAGES).astype(jnp.int32)
    directions = unit_rows(jax.random.normal(jax.random.fold_in(key, 102), (PASSAGES, DIM), jnp.float32) * first_half)
    query_common = unit_rows(jax.random.normal(jax.random.fold_in(key, 103), (DIM,), jnp.float32) * second_half)
    passage_common = unit_rows(jax.random.normal(jax.random.fold_in(key, 104), (DIM,), jnp.float32) * second_half)
    return (chosen, directions, query_common, passage_common, first_half, second_half)


def draw_positive(key, part):
    return shared_parts(key)[0]


def draw_query_emb(key, part):
    chosen, directions, query_common, passage_common, first_half, second_half = shared_parts(key)
    spread = noise_level * DIM ** (-0.25) * (second_half + 0.25 * first_half)
    noise_key = jax.random.fold_in(key, 201)
    noise = jax.random.normal(noise_key, (QUERIES, QLEN, DIM), jnp.float32)
    common = query_common
    aligned = similar_gap / QLEN * directions[chosen]
    values = noise * spread + common + aligned[:, None, :]
    return jnp.clip(values, -6.0, 6.0).astype(jnp.bfloat16)


def draw_passage_emb(key, part):
    chosen, directions, query_common, passage_common, first_half, second_half = shared_parts(key)
    spread = noise_level * DIM ** (-0.25)
    noise_key = jax.random.fold_in(key, 301)
    noise = jax.random.normal(noise_key, (PASSAGES, PLEN, DIM), jnp.float32)
    common = passage_common
    values = noise * spread + common + directions[:, None, :]
    return jnp.clip(values, -6.0, 6.0).astype(jnp.bfloat16)


def touch_ends(entries, key, least, high):
    index_at = [jax.random.randint(jax.random.fold_in(key, axis), (), 0, length) for axis, length in enumerate(entries.shape)]
    widest = entries.shape.index(max(entries.shape))
    beside = index_at[:widest] + [(index_at[widest] + 1) % entries.shape[widest]] + index_at[widest + 1:]
    return entries.at[tuple(index_at)].set(least).at[tuple(beside)].set(high)


def levels(key, extent, split, smallest, high):
    def one(position, parts):
        heights = jax.random.uniform(jax.random.fold_in(jax.random.fold_in(key, 6), position), (parts,), jnp.float32, smallest / len(split), high / len(split))
        return jnp.repeat(jnp.exp(heights), extent[position] // parts).reshape((-1,) + (1,) * (len(extent) - position - 1))

    loudness = one(*split[0])
    for cut in split[1:]:
        loudness = loudness * one(*cut)
    return loudness


def bell_draw(key, extent, scale, most, split=(), dtype=jnp.bfloat16):
    loudness = levels(key, extent, split, -0.22, 0.18) if split else 1.0
    entries = jax.random.normal(key, extent, jnp.float32) * scale * loudness
    return jnp.minimum(jnp.maximum(entries, -most), most).astype(dtype)


def setup_inputs(seed: int = 0) -> dict:
    key_list = jax.random.split(jax.random.key(seed), 10)
    query_emb = draw_query_emb(jax.random.fold_in(key_list[9], 71), 0)
    positive = draw_positive(jax.random.fold_in(key_list[9], 71), 0)
    passage_emb = draw_passage_emb(jax.random.fold_in(key_list[9], 71), 0)
    lengths = touch_ends(jax.random.randint(key_list[3], (PASSAGES,), PLEN // 2, PLEN + 1), jax.random.fold_in(key_list[3], 1), PLEN // 2, PLEN).astype(jnp.int32)
    residual = bell_draw(key_list[4], (ROWS, D), 1.0, 6.0, ((0, 32),))
    context = bell_draw(key_list[5], (ROWS, D), 1.0, 6.0, ((0, 32),))
    out_proj = bell_draw(key_list[6], (D, D), D ** -0.5, 0.1875)
    norm_gain = jnp.clip(1.0 + 0.1 * jax.random.normal(key_list[7], (D,), jnp.float32), 0.5, 1.5)
    colbert_proj = bell_draw(key_list[8], (D, DIM), D ** -0.5, 0.1875)
    return {"query_emb": query_emb, "positive": positive, "passage_emb": passage_emb, "lengths": lengths, "residual": residual, "context": context, "out_proj": out_proj, "norm_gain": norm_gain, "colbert_proj": colbert_proj}


def masked_scores(query_flat, passage_tokens, length):
    scores = jnp.dot(query_flat, passage_tokens.T, preferred_element_type=jnp.float32)
    usable = (jnp.arange(passage_tokens.shape[0]) < length)[None, :]
    return jnp.where(usable, scores, -1e+30)

def window_rows(running, inputs, out_proj, norm_gain, colbert_proj):
    resid_rows, context_rows, grad_rows = inputs
    hidden = resid_rows.astype(jnp.float32) + jnp.dot(context_rows, out_proj, preferred_element_type=jnp.float32)
    row_mean = lax.optimization_barrier(jnp.mean(hidden, axis=1, keepdims=True))
    centred = hidden - row_mean
    variance = lax.optimization_barrier(jnp.mean(centred * centred, axis=1, keepdims=True))
    inv_std = 1.0 / jnp.sqrt(variance + 1e-05)
    normed = centred * inv_std
    scaled = (normed * norm_gain).astype(jnp.bfloat16)
    colbert_part = jnp.dot(scaled.T, grad_rows, preferred_element_type=jnp.float32)
    scaled_grad = jnp.dot(grad_rows, colbert_proj.T, preferred_element_type=jnp.float32)
    gain_part = lax.optimization_barrier(jnp.sum(scaled_grad * normed, axis=0))
    gained = scaled_grad * norm_gain
    hidden_grad = (inv_std * (gained - lax.optimization_barrier(jnp.mean(gained, axis=1, keepdims=True)) - normed * lax.optimization_barrier(jnp.mean(gained * normed, axis=1, keepdims=True)))).astype(jnp.bfloat16)
    context_grad = jnp.dot(hidden_grad, out_proj.T, preferred_element_type=jnp.float32).astype(jnp.bfloat16)
    proj_part = jnp.dot(context_rows.T, hidden_grad, preferred_element_type=jnp.float32)
    running = (running[0] + proj_part, running[1] + colbert_part, running[2] + gain_part)
    return (running, (hidden_grad, context_grad))

def reference(query_emb, positive, passage_emb, lengths, residual, context, out_proj, norm_gain, colbert_proj):
    query_flat = query_emb.reshape(QUERIES * QLEN, DIM)

    def forward(inputs):
        passage_tokens, length = inputs
        masked = masked_scores(query_flat, passage_tokens, length)
        highest = lax.optimization_barrier(jnp.max(masked, axis=1, keepdims=True))
        inner_lse = highest[:, 0] + jnp.log(lax.optimization_barrier(jnp.sum(jnp.exp(masked - highest), axis=1)))
        shifted = inner_lse - jnp.log(length.astype(jnp.float32))
        return (inner_lse, lax.optimization_barrier(jnp.sum(shifted.reshape(QUERIES, QLEN), axis=1)))
    inner_all, similar = lax.map(forward, (passage_emb, lengths))
    similar = similar.T
    highest = lax.optimization_barrier(jnp.max(similar, axis=1, keepdims=True))
    log_total = highest[:, 0] + jnp.log(lax.optimization_barrier(jnp.sum(jnp.exp(similar - highest), axis=1)))
    is_positive = jnp.arange(PASSAGES).astype(jnp.int32)[None, :] == positive[:, None]
    positive_score = lax.optimization_barrier(jnp.sum(jnp.where(is_positive, similar, 0.0), axis=1))
    loss = jnp.mean(log_total - positive_score)
    coefficient = jnp.exp(similar - log_total[:, None]) - is_positive.astype(jnp.float32)

    def backward(running, inputs):
        passage_tokens, length, inner_lse, column = inputs
        masked = masked_scores(query_flat, passage_tokens, length)
        spread = jnp.exp(masked - inner_lse[:, None]).reshape(QUERIES, QLEN, PLEN)
        weight = (spread * column[:, None, None]).reshape(QUERIES * QLEN, PLEN).astype(jnp.bfloat16)
        running = running + jnp.dot(weight, passage_tokens, preferred_element_type=jnp.float32)
        passage_grad = jnp.dot(weight.T, query_flat, preferred_element_type=jnp.float32).astype(jnp.bfloat16)
        return (running, passage_grad)
    start = jnp.zeros((QUERIES * QLEN, DIM), jnp.float32)
    query_sum, emb_grad = lax.scan(backward, start, (passage_emb, lengths, inner_all, coefficient.T))
    query_grad = query_sum.reshape(QUERIES, QLEN, DIM)

    def window_step(running, inputs):
        return window_rows(running, inputs, out_proj, norm_gain, colbert_proj)
    begin = (jnp.zeros((D, D), jnp.float32), jnp.zeros((D, DIM), jnp.float32), jnp.zeros((D,), jnp.float32))
    sums, grads = lax.scan(window_step, begin, (residual.reshape(PASSAGES, PLEN, D), context.reshape(PASSAGES, PLEN, D), emb_grad))
    residual_grad = grads[0].reshape(ROWS, D)
    context_grad = grads[1].reshape(ROWS, D)
    return (loss, query_grad, residual_grad, context_grad, sums[0], sums[1], sums[2])
```

```python
import functools

import jax
import jax.numpy as jnp
from jax import lax
from jax.experimental import pallas as pl
from jax.experimental.pallas import tpu as pltpu
from jax.sharding import PartitionSpec as P

MESH = pl.DeviceIdType.MESH
VMEM = pl.BlockSpec(memory_space=pltpu.VMEM)
LANES = 128
LOW = -1e30


def place(axis, size, step):
    there = lax.rem(lax.axis_index(axis) + step + size, size)
    if axis == "dp":
        return (there, lax.axis_index("neg"))
    return (lax.axis_index("dp"), there)


def greet(sizes):
    barrier = pltpu.get_barrier_semaphore()
    for axis, size in sizes:

        def tell(k, carry):
            pl.semaphore_signal(
                barrier, inc=1, device_id=place(axis, size, k), device_id_type=MESH
            )
            return carry

        lax.fori_loop(1, size, tell, 0)
    pl.semaphore_wait(barrier, sum(size - 1 for _, size in sizes))


def remote(src, dst, send, recv, device):
    return pltpu.make_async_remote_copy(
        src_ref=src, dst_ref=dst, send_sem=send, recv_sem=recv, device_id=device, device_id_type=MESH
    )


def each(size, act):
    def turn(k, carry):
        act(k)
        return carry

    lax.fori_loop(1, size, turn, 0)


def gather_kernel(sizes, plan, *refs):
    count = len(plan)
    ins, outs, sems = refs[:count], refs[count : 2 * count], refs[2 * count :]
    greet([(axis, sizes[axis]) for axis in dict.fromkeys(plan)])
    for i, axis in enumerate(plan):
        me = lax.axis_index(axis)
        each(
            sizes[axis],
            lambda k: remote(
                ins[i], outs[i].at[me], sems[2 * i].at[k], sems[2 * i + 1].at[k], place(axis, sizes[axis], k)
            ).start(),
        )
    for i, axis in enumerate(plan):
        outs[i][lax.axis_index(axis)] = ins[i][...]
    for i, axis in enumerate(plan):
        size = sizes[axis]
        me = lax.axis_index(axis)

        def finish(k):
            slot = lax.rem(me - k + size, size)
            copy = remote(
                ins[i], outs[i].at[slot], sems[2 * i].at[k], sems[2 * i + 1].at[k], place(axis, size, k)
            )
            copy.wait_recv()
            copy.wait_send()

        each(size, finish)


def gather(sizes, ident, pairs):
    plan = tuple(axis for _, axis in pairs)
    arrays = [array for array, _ in pairs]
    sems = []
    for axis in plan:
        sems += [pltpu.SemaphoreType.DMA((sizes[axis],))] * 2
    return pl.pallas_call(
        functools.partial(gather_kernel, sizes, plan),
        out_shape=[
            jax.ShapeDtypeStruct((sizes[axis],) + array.shape, array.dtype) for array, axis in pairs
        ],
        in_specs=[VMEM] * len(plan),
        out_specs=[VMEM] * len(plan),
        scratch_shapes=sems,
        compiler_params=pltpu.CompilerParams(collective_id=ident, has_side_effects=True),
    )(*arrays)


def scatter_kernel(sizes, plan, *refs):
    count = len(plan)
    ins, outs, rest = refs[:count], refs[count : 2 * count], refs[2 * count :]
    lands, sems = rest[:count], rest[count:]
    greet([(axis, sizes[axis]) for axis in plan])
    for i, axis in enumerate(plan):
        size = sizes[axis]
        me = lax.axis_index(axis)

        each(
            size,
            lambda k: remote(
                ins[i].at[lax.rem(me + k, size)],
                lands[i].at[k],
                sems[2 * i].at[k],
                sems[2 * i + 1].at[k],
                place(axis, size, k),
            ).start(),
        )
    for i, axis in enumerate(plan):
        size = sizes[axis]
        me = lax.axis_index(axis)

        def finish(k):
            copy = remote(
                ins[i].at[lax.rem(me + k, size)],
                lands[i].at[k],
                sems[2 * i].at[k],
                sems[2 * i + 1].at[k],
                place(axis, size, k),
            )
            copy.wait_recv()
            copy.wait_send()

        each(size, finish)
        total = ins[i][me].astype(jnp.float32)
        for k in range(1, size):
            total = total + lands[i][k].astype(jnp.float32)
        outs[i][...] = total.astype(outs[i].dtype)


def scatter(sizes, ident, triples):
    plan = tuple(axis for _, axis, _ in triples)
    sems, lands = [], []
    for array, axis, _ in triples:
        lands.append(pltpu.VMEM(array.shape, array.dtype))
        sems += [pltpu.SemaphoreType.DMA((sizes[axis],))] * 2
    return pl.pallas_call(
        functools.partial(scatter_kernel, sizes, plan),
        out_shape=[jax.ShapeDtypeStruct(array.shape[1:], dtype) for array, _, dtype in triples],
        in_specs=[VMEM] * len(plan),
        out_specs=[VMEM] * len(plan),
        scratch_shapes=lands + sems,
        compiler_params=pltpu.CompilerParams(collective_id=ident, has_side_effects=True),
    )(*[array for array, _, _ in triples])


def total_kernel(dp, neg, part, gain, extra, out, small, pair_in, held, lands, mine, pair_small, all_small,
                 pair_s, pair_r, rs_s, rs_r, ag_s, ag_r, fw_s, fw_r, sm_s, sm_r, sp_s, sp_r):
    groups = neg // 2
    n = dp * groups
    row, col = lax.axis_index("dp"), lax.axis_index("neg")
    core = lax.rem(col, 2)
    other = 1 - core
    me = row * groups + col // 2
    partner = (row, col + 1 - 2 * core)

    def at(k):
        return lax.rem(me + k + n, n)

    def device(k):
        t = at(k)
        return (t // groups, lax.rem(t, groups) * 2 + core)

    barrier = pltpu.get_barrier_semaphore()
    pl.semaphore_signal(barrier, inc=1, device_id=partner, device_id_type=MESH)
    each(n, lambda k: pl.semaphore_signal(barrier, inc=1, device_id=device(k), device_id_type=MESH))
    pl.semaphore_wait(barrier, n)

    wide = gain.shape[1]
    mine[:, :wide] = gain[...]
    mine[:, wide:] = extra[...]

    def pair_copy(k):
        return remote(part.at[other, at(k)], pair_in.at[at(k)], pair_s.at[k], pair_r.at[k], partner)

    def rs_copy(k):
        return remote(held.at[at(k)], lands.at[k], rs_s.at[k], rs_r.at[k], device(k))

    each(n, lambda k: pair_copy(k).start())
    pair_copy(0).start()
    sp_copy = remote(mine, pair_small, sp_s, sp_r, partner)
    sp_copy.start()

    def join(k):
        pair_copy(k).wait_recv()
        t = at(k)
        held[t] = (part[core, t].astype(jnp.float32) + pair_in[t].astype(jnp.float32)).astype(held.dtype)

    def join_send(k):
        join(k)
        rs_copy(k).start()

    each(n, join_send)
    join(0)
    sp_copy.wait_recv()
    all_small[me] = mine[...] + pair_small[...]

    def sm_copy(k, slot):
        return remote(all_small.at[slot], all_small.at[slot], sm_s.at[k], sm_r.at[k], device(k))

    each(n, lambda k: sm_copy(k, me).start())

    def add(k, total):
        rs_copy(k).wait_recv()
        return total + lands[k].astype(jnp.float32)

    total = lax.fori_loop(1, n, add, held[me].astype(jnp.float32))
    out[core, me] = total.astype(out.dtype)

    def ag_copy(k, slot):
        return remote(out.at[core, slot], out.at[core, slot], ag_s.at[k], ag_r.at[k], device(k))

    def fw_copy(k, half):
        return remote(out.at[half, at(-k)], out.at[half, at(-k)], fw_s.at[k], fw_r.at[k], partner)

    each(n, lambda k: ag_copy(k, me).start())
    fw_copy(0, core).start()

    def pass_on(k):
        ag_copy(k, at(-k)).wait_recv()
        fw_copy(k, core).start()

    each(n, pass_on)
    each(n, lambda k: sm_copy(k, at(-k)).wait_recv())

    def add_small(k, so_far):
        return so_far + all_small[k]

    small[...] = lax.fori_loop(1, n, add_small, all_small[0])

    def drain(k):
        fw_copy(k, other).wait_recv()
        fw_copy(k, core).wait_send()
        pair_copy(k).wait_send()

    drain(0)
    sp_copy.wait_send()

    def drain_all(k):
        drain(k)
        rs_copy(k).wait_send()
        ag_copy(k, me).wait_send()
        sm_copy(k, me).wait_send()

    each(n, drain_all)


def total_sum(sizes, ident, part, gain, extra):
    dp, neg = sizes["dp"], sizes["neg"]
    n = dp * neg // 2
    rows, columns = part.shape
    part = part.reshape(2, n, rows // (2 * n), columns)
    piece = part.shape[1:]
    width = gain.shape[1] + extra.shape[1]
    dma = pltpu.SemaphoreType.DMA
    out, small = pl.pallas_call(
        functools.partial(total_kernel, dp, neg),
        out_shape=[
            jax.ShapeDtypeStruct(part.shape, part.dtype),
            jax.ShapeDtypeStruct((1, width), jnp.float32),
        ],
        in_specs=[VMEM] * 3,
        out_specs=[VMEM] * 2,
        scratch_shapes=[
            pltpu.VMEM(piece, part.dtype),
            pltpu.VMEM(piece, part.dtype),
            pltpu.VMEM(piece, part.dtype),
            pltpu.VMEM((1, width), jnp.float32),
            pltpu.VMEM((1, width), jnp.float32),
            pltpu.VMEM((n, 1, width), jnp.float32),
        ]
        + [dma((n,))] * 10
        + [dma] * 2,
        compiler_params=pltpu.CompilerParams(collective_id=ident, has_side_effects=True),
    )(part, gain, extra)
    return out.reshape(rows, columns), small


def select_tokens(rows, queries, per):
    token = lax.broadcasted_iota(jnp.int32, (rows, queries), 0)
    query = lax.broadcasted_iota(jnp.int32, (rows, queries), 1)
    return jnp.where(token // per == query, 1.0, 0.0)


def masked(passage, queries, length):
    scores = lax.dot_general(
        passage, queries, (((1,), (1,)), ((), ())), preferred_element_type=jnp.float32
    )
    position = lax.broadcasted_iota(jnp.int32, scores.shape, 0)
    return jnp.where(position < length, scores, LOW)


def forward_kernel(per, queries, passages, lengths, inner, similar):
    slots = passages.shape[0]
    tokens = queries.shape[0]
    inner[...] = jnp.zeros_like(inner)
    wide = tokens // 4 if tokens % 512 == 0 else tokens

    def one(p, carry):
        length = lengths[p, 0:1, 0:1]
        for start in range(0, tokens, wide):
            scores = masked(passages[p], queries[start : start + wide, :], length)
            highest = jnp.max(scores, axis=0, keepdims=True)
            lse = highest + jnp.log(jnp.sum(jnp.exp(scores - highest), axis=0, keepdims=True))
            inner[pl.ds(p, 1), start : start + wide] = lse
        return carry

    lax.fori_loop(0, slots, one, 0)
    chosen = select_tokens(tokens, similar.shape[1], per)
    summed = jnp.dot(
        inner[...], chosen, precision=lax.Precision.HIGHEST, preferred_element_type=jnp.float32
    )
    similar[...] = jnp.full_like(similar, LOW)
    for p in range(slots):
        shift = jnp.log(lengths[p, 0:1, 0:1].astype(jnp.float32)) * per
        similar[p : p + 1, :] = summed[p : p + 1, :] - shift


def backward_kernel(per, own, queries, passages, lengths, positives, inner, similar, everyone,
                    query_part, passage_part, loss_row, spread_coef, running):
    slots = passages.shape[0]
    tokens = queries.shape[0]
    neg = everyone.shape[0]
    here = lax.axis_index("neg")
    positive = positives[0]
    for s in range(1, neg):
        positive = positive + positives[s]
    positive = positive[0:1, :]
    highest = jnp.max(jnp.max(everyone[...], axis=0), axis=0, keepdims=True)
    row = lax.broadcasted_iota(jnp.int32, similar.shape, 0)
    exp_total = jnp.zeros(similar.shape, jnp.float32)
    score = jnp.zeros(similar.shape, jnp.float32)
    for s in range(neg):
        exp_total = exp_total + jnp.exp(everyone[s] - highest)
        score = score + jnp.where((row * neg + s == positive) & (row < slots), everyone[s], 0.0)
    log_total = highest + jnp.log(jnp.sum(exp_total, axis=0, keepdims=True))
    score = jnp.sum(score, axis=0, keepdims=True)
    lane = lax.broadcasted_iota(jnp.int32, log_total.shape, 1)
    mine = (lane >= here * own) & (lane < here * own + own)
    loss_row[...] = jnp.where(mine, log_total - score, 0.0)
    hit = jnp.where((row * neg + here == positive) & (row < slots), 1.0, 0.0)
    used = (row < slots) & (lax.broadcasted_iota(jnp.int32, similar.shape, 1) < tokens // per)
    coefficient = jnp.where(used, jnp.exp(similar[...] - log_total) - hit, 0.0)
    chosen = select_tokens(tokens, similar.shape[1], per)
    spread_coef[...] = lax.dot_general(
        coefficient, chosen, (((1,), (1,)), ((), ())),
        precision=lax.Precision.HIGHEST, preferred_element_type=jnp.float32,
    )
    running[...] = jnp.zeros_like(running)
    wide = tokens // 4 if tokens % 512 == 0 else tokens

    def one(p, carry):
        length = lengths[p, 0:1, 0:1]
        passage = passages[p]
        flipped = passage.astype(jnp.float32).T.astype(passage.dtype)
        total = jnp.zeros(passage.shape, jnp.float32)
        for start in range(0, tokens, wide):
            block = queries[start : start + wide, :]
            scores = masked(passage, block, length)
            spread = jnp.exp(scores - inner[pl.ds(p, 1), start : start + wide])
            weight = (spread * spread_coef[pl.ds(p, 1), start : start + wide]).astype(jnp.bfloat16)
            running[:, start : start + wide] += jnp.dot(
                flipped, weight, preferred_element_type=jnp.float32
            )
            total = total + jnp.dot(weight, block, preferred_element_type=jnp.float32)
        passage_part[p] = total.astype(passage_part.dtype)
        return carry

    lax.fori_loop(0, slots, one, 0)
    query_part[...] = running[...].T.astype(query_part.dtype)


def window_rows(resid_rows, context_rows, grad_rows, out_proj, norm_gain, colbert_proj):
    hidden = resid_rows.astype(jnp.float32) + jnp.dot(
        context_rows, out_proj, preferred_element_type=jnp.float32
    )
    row_mean = jnp.mean(hidden, axis=1, keepdims=True)
    centred = hidden - row_mean
    variance = jnp.mean(centred * centred, axis=1, keepdims=True)
    inv_std = 1.0 / jnp.sqrt(variance + 1e-05)
    normed = centred * inv_std
    scaled = (normed * norm_gain).astype(jnp.bfloat16)
    colbert_part = jnp.dot(scaled.T, grad_rows, preferred_element_type=jnp.float32)
    scaled_grad = jnp.dot(grad_rows, colbert_proj.T, preferred_element_type=jnp.float32)
    gain_part = jnp.sum(scaled_grad * normed, axis=0)
    gained = scaled_grad * norm_gain
    hidden_grad = (
        inv_std
        * (
            gained
            - jnp.mean(gained, axis=1, keepdims=True)
            - normed * jnp.mean(gained * normed, axis=1, keepdims=True)
        )
    ).astype(jnp.bfloat16)
    context_grad = jnp.dot(hidden_grad, out_proj.T, preferred_element_type=jnp.float32).astype(
        jnp.bfloat16
    )
    proj_part = jnp.dot(context_rows.T, hidden_grad, preferred_element_type=jnp.float32)
    return (hidden_grad, context_grad, proj_part, colbert_part, gain_part)


def body(sizes, query_emb, positive, passage_emb, lengths, residual, context, out_proj, norm_gain, colbert_proj):
    dp, neg = sizes["dp"], sizes["neg"]
    own, per, dim = query_emb.shape
    slots, plen = dp * passage_emb.shape[0], passage_emb.shape[1]
    group = own * neg
    tokens = group * per
    lanes = -(-group // LANES) * LANES
    rows = -(-slots // 8) * 8
    here = lax.axis_index("neg")
    pos_row = lax.dynamic_update_slice(jnp.zeros((8, lanes), jnp.int32), jnp.broadcast_to(positive, (8, own)), (0, here * own))
    len_row = jnp.broadcast_to(lengths, (8, LANES))
    queries, positives, passages, lens = gather(
        sizes,
        1,
        [
            (query_emb.reshape(own * per, dim), "neg"),
            (pos_row, "neg"),
            (passage_emb.reshape(plen, dim), "dp"),
            (len_row, "dp"),
        ],
    )
    queries = queries.reshape(tokens, dim)
    inner, similar = pl.pallas_call(
        functools.partial(forward_kernel, per),
        out_shape=[
            jax.ShapeDtypeStruct((rows, tokens), jnp.float32),
            jax.ShapeDtypeStruct((rows, lanes), jnp.float32),
        ],
        in_specs=[VMEM] * 3,
        out_specs=[VMEM] * 2,
    )(queries, passages, lens)
    (everyone,) = gather(sizes, 2, [(similar, "neg")])
    query_part, passage_part, loss_row = pl.pallas_call(
        functools.partial(backward_kernel, per, own),
        out_shape=[
            jax.ShapeDtypeStruct((tokens, dim), jnp.bfloat16),
            jax.ShapeDtypeStruct((slots, plen, dim), jnp.bfloat16),
            jax.ShapeDtypeStruct((1, lanes), jnp.float32),
        ],
        in_specs=[VMEM] * 7,
        out_specs=[VMEM] * 3,
        scratch_shapes=[pltpu.VMEM((rows, tokens), jnp.float32), pltpu.VMEM((dim, tokens), jnp.float32)],
    )(queries, passages, lens, positives, inner, similar, everyone)
    query_grad, emb_grad = scatter(
        sizes,
        3,
        [
            (query_part.reshape(neg, own * per, dim), "neg", jnp.float32),
            (passage_part, "dp", jnp.bfloat16),
        ],
    )
    residual_grad, context_grad, proj_part, colbert_part, gain_part = window_rows(
        residual, context, emb_grad, out_proj, norm_gain, colbert_proj
    )
    part = jnp.concatenate([proj_part.astype(jnp.bfloat16), colbert_part.astype(jnp.bfloat16)], axis=1)
    summed, small = total_sum(sizes, 4, part, gain_part[None, :], loss_row)
    width = norm_gain.shape[0]
    loss = jnp.sum(small[0, width:]) / (own * dp * neg)
    return (
        loss,
        query_grad.reshape(own, per, dim),
        residual_grad,
        context_grad,
        summed[:, :width].astype(jnp.float32),
        summed[:, width:].astype(jnp.float32),
        small[0, :width],
    )


def solution(mesh):
    sizes = {axis: mesh.shape[axis] for axis in ("dp", "neg")}
    split = ("dp", "neg")
    in_specs = (
        P(split, None, None),
        P(split),
        P(split, None, None),
        P(split),
        P(split, None),
        P(split, None),
        P(),
        P(),
        P(),
    )
    out_specs = (
        P(),
        P(split, None, None),
        P(split, None),
        P(split, None),
        P(),
        P(),
        P(),
    )
    return jax.shard_map(
        functools.partial(body, sizes), mesh=mesh, in_specs=in_specs, out_specs=out_specs, check_vma=False
    )
```
